32 devices in a mesh: parts: 2 (over y), row: 16 (over z, x, core).
Axes of the slice: x: 2, y: 2, z: 4, core: 2. Of those that a mesh axis runs over, the one named last changes fastest.
Arguments:
- object_tile: float32 [2, 8192, 256], P(None, ('parts', 'row')), parts along dimension 1, may hold values from -6 to 6
- probe_modes: float32 [2, 4, 128, 128], replicated, may hold values from -4 to 4
- measured: float32 [128, 128, 128], P(('parts', 'row')), parts along dimension 0, may hold values from 0.5 to 8
- offsets: int32 [128, 2], P(('parts', 'row')), parts along dimension 0, may hold values from -64 to 192, as said below
- counts: int32 [32], P(('parts', 'row')), parts along dimension 0, may hold values from 2 to 4, as said below
Outputs:
- object_out: float32 [2, 8192, 256], P(None, ('parts', 'row')), parts along dimension 1
- probe_out: float32 [4, 4, 128, 128], P('parts'), parts along dimension 0
The draws below stay inside these ranges and needn't reach their ends.
There are 2 independent parts, one for each index of `parts`. The reference program is written for one: setup_inputs(seed, part) draws one part's arguments, and reference() takes and returns one part's arrays. A program takes and returns all parts, laid end to end along the dimension named above; an argument that names none is the same for every part. Nothing has to cross between parts.
Inputs may be any that keep to these rules, and one draw needn't show every extreme that they name: `offsets`: column 0 is a row offset relative to the tile's first row, from -64 to 192; in every tile the first slot has -64 and the second 256 - 64; column 1 is a column offset from 0 to 128. counts[t] live slots of tile t come first, the others are unused; some tile has 4.
All inputs are finite; a program needn't handle non-finite values.
Results may differ from the reference program's by a relative error of at most 0.0003.
Values sent between devices are 32-bit elements; how exact they have to be, the bound alone decides.
A program may use at most 64 MiB of HBM per device.

```python
import math
import jax
import jax.numpy as jnp
from jax import lax

W = 128
MODES = 4
MARGIN = 64
TILE = 256
P_MAX = 4
ITERS = 2
OBJ_ROWS = 4096
SLOTS = 64
N_ROW = 16


def draw_object_tile(key, part):
    first = jax.random.fold_in(jax.random.fold_in(key, 5), 0)
    ramp = 0.5 + jnp.arange(OBJ_ROWS, dtype=jnp.float32) / OBJ_ROWS
    base = jax.random.truncated_normal(first, -4.0, 4.0, (2, OBJ_ROWS, TILE), jnp.float32)
    return base * ramp[None, :, None]


def draw_offsets(key, part):
    first, second = jax.random.split(jax.random.fold_in(key, 23))
    row_offset = jax.random.randint(first, (SLOTS,), 0 - MARGIN, TILE - W + MARGIN + 1)
    col_offset = jax.random.randint(second, (SLOTS,), 0, TILE - W + 1)
    within = jnp.arange(SLOTS, dtype=jnp.int32) % P_MAX
    row_offset = jnp.where(within == 0, 0 - MARGIN, row_offset)
    row_offset = jnp.where(within == 1, TILE - W + MARGIN, row_offset)
    return jnp.stack([row_offset, col_offset], axis=1).astype(jnp.int32)


def draw_counts(key, part):
    first, second, third = jax.random.split(jax.random.fold_in(key, 11), 3)
    light = jax.random.randint(first, (N_ROW,), 2, max(P_MAX // 2, 2) + 1)
    heavy = jax.random.randint(second, (N_ROW,), 0, 8) == 0
    chosen = jax.random.randint(third, (), 0, N_ROW)
    result = jnp.where(heavy, P_MAX, light)
    result = jnp.where(jnp.arange(N_ROW) == chosen, P_MAX, result)
    return result.astype(jnp.int32)


def levels(stream_key, extent, shards, low, largest):
    level, own = 1.0, jax.random.fold_in(stream_key, 6)
    for dim, blocks in shards:
        draws = jnp.exp(jax.random.uniform(jax.random.fold_in(own, dim), (blocks,), jnp.float32, low / len(shards), largest / len(shards)))
        level = level * jnp.repeat(draws, extent[dim] // blocks).reshape([-1 if axis == dim else 1 for axis in range(len(extent))])
    return level


def normal_values(stream_key, dims, deviation, limit, kind=jnp.bfloat16):
    values = jax.random.normal(stream_key, dims, jnp.float32) * deviation
    return jnp.minimum(jnp.maximum(values, -limit), limit).astype(kind)


def setup_inputs(seed: int = 0, part: int = 0) -> dict:
    seeds = jax.random.split(jax.random.key(seed), 6)
    part_splits = jax.random.split(jax.random.fold_in(seeds[5], part), 6)
    return {
        "object_tile": draw_object_tile(jax.random.fold_in(jax.random.fold_in(seeds[5], part), 71), part),
        "probe_modes": normal_values(seeds[1], (2, MODES, W, W), 0.7, 4.0, jnp.float32),
        "measured": jnp.clip(jnp.exp(math.log(8.0) - 2.7725887 * jax.random.uniform(part_splits[2], (SLOTS, W, W), jnp.float32) ** levels(part_splits[2], (SLOTS, W, W), ((0, 16),), -0.2, 0.2)), 0.5, 8.0),
        "offsets": draw_offsets(jax.random.fold_in(jax.random.fold_in(seeds[5], part), 71), part),
        "counts": draw_counts(jax.random.fold_in(jax.random.fold_in(seeds[5], part), 71), part),
    }


object_rate = 0.2
probe_rate = 0.5

def dft_tables(length):
    index = jnp.arange(length, dtype=jnp.int32)
    product = index[:, None] * index[None, :] % length
    phase = 2.0 * math.pi / length * product.astype(jnp.float32)
    factor = 1.0 / math.sqrt(length)
    return (jnp.cos(phase) * factor, -jnp.sin(phase) * factor)

def transform(real_part, imag_part, cosine_table, sine_table, direction):
    highest = lax.Precision.HIGHEST
    signed = direction * sine_table
    left_real = jnp.einsum('ab,mbc->mac', cosine_table, real_part, precision=highest) - jnp.einsum('ab,mbc->mac', signed, imag_part, precision=highest)
    left_imag = jnp.einsum('ab,mbc->mac', cosine_table, imag_part, precision=highest) + jnp.einsum('ab,mbc->mac', signed, real_part, precision=highest)
    out_real = jnp.einsum('mab,bc->mac', left_real, cosine_table, precision=highest) - jnp.einsum('mab,bc->mac', left_imag, signed, precision=highest)
    out_imag = jnp.einsum('mab,bc->mac', left_imag, cosine_table, precision=highest) + jnp.einsum('mab,bc->mac', left_real, signed, precision=highest)
    return (out_real, out_imag)

def position_terms(window, probe_now, target, live, cosine_table, sine_table):
    probe_real, probe_imag = (probe_now[0], probe_now[1])
    window_real, window_imag = (window[0], window[1])
    exit_real = probe_real * window_real - probe_imag * window_imag
    exit_imag = probe_real * window_imag + probe_imag * window_real
    far_real, far_imag = transform(exit_real, exit_imag, cosine_table, sine_table, 1.0)
    intensity = lax.optimization_barrier(jnp.sum(far_real * far_real + far_imag * far_imag, axis=0))
    resid = (intensity - target) * live
    back_real, back_imag = transform(resid * far_real, resid * far_imag, cosine_table, sine_table, -1.0)
    grad_real = lax.optimization_barrier(jnp.sum(probe_real * back_real + probe_imag * back_imag, axis=0))
    grad_imag = lax.optimization_barrier(jnp.sum(probe_real * back_imag - probe_imag * back_real, axis=0))
    probe_term_real = window_real * back_real + window_imag * back_imag
    probe_term_imag = window_real * back_imag - window_imag * back_real
    energy_term = live * jnp.sum(window_real * window_real + window_imag * window_imag)
    return (jnp.stack([grad_real, grad_imag]), jnp.stack([probe_term_real, probe_term_imag]), energy_term)

def reference(object_tile, probe_modes, measured, offsets, counts):
    cosine_table, sine_table = dft_tables(W)
    slots = jnp.arange(SLOTS, dtype=jnp.int32)
    owners = slots // P_MAX
    live_all = (slots % P_MAX < counts[owners]).astype(jnp.float32)
    current = object_tile
    probe_now = probe_modes
    for sweep_index in range(ITERS):
        padded = jnp.pad(current, ((0, 0), (MARGIN, MARGIN), (0, 0)))

        def visit(carry, item):
            gradient, probe_grad, energy = carry
            slot, owner, live = item
            zero = jnp.zeros((), jnp.int32)
            row_start = (owner * TILE + offsets[slot, 0] + MARGIN).astype(jnp.int32)
            col_start = offsets[slot, 1].astype(jnp.int32)
            window = lax.dynamic_slice(padded, (zero, row_start, col_start), (2, W, W))
            window_grad, probe_term, energy_term = position_terms(window, probe_now, measured[slot], live, cosine_table, sine_table)
            present = lax.dynamic_slice(gradient, (zero, row_start, col_start), (2, W, W))
            gradient = lax.dynamic_update_slice(gradient, present + window_grad, (zero, row_start, col_start))
            return ((gradient, probe_grad + probe_term, energy + energy_term), None)
        start = (jnp.zeros_like(padded), jnp.zeros_like(probe_now), jnp.zeros((), jnp.float32))
        (gradient, probe_grad, energy), unused = lax.scan(visit, start, (slots, owners, live_all))
        object_step = object_rate / jnp.max(lax.optimization_barrier(jnp.sum(probe_now[0] * probe_now[0] + probe_now[1] * probe_now[1], axis=0)))
        probe_step = probe_rate * W * W / energy
        current = current - object_step * gradient[:, MARGIN:MARGIN + OBJ_ROWS]
        probe_now = probe_now - probe_step * probe_grad
    return (current, probe_now)
```

```python
import functools
import math

import jax
import jax.numpy as jnp
import numpy as np
from jax import lax
from jax.experimental import pallas as pl
from jax.experimental.pallas import tpu as pltpu
from jax.sharding import PartitionSpec as P

ITERS = 2
object_rate = 0.2
probe_rate = 0.5
ENERGY_ROWS = 8
VMEM = pl.BlockSpec(memory_space=pltpu.VMEM)
SMEM = pl.BlockSpec(memory_space=pltpu.SMEM)
MESH = pl.DeviceIdType.MESH


def dft_tables(length):
    index = np.arange(length)
    phase = 2.0 * math.pi / length * (index[:, None] * index[None, :] % length)
    cosine = np.cos(phase) / math.sqrt(length)
    sine = -np.sin(phase) / math.sqrt(length)
    forward = np.block([[cosine, -sine], [sine, cosine]]).astype(np.float32)
    backward = np.block([[cosine, sine], [-sine, cosine]]).astype(np.float32)
    tables = []
    for table in (forward, backward):
        high = table.astype(jnp.bfloat16)
        low = (table - high.astype(np.float32)).astype(jnp.bfloat16)
        tables.append(jnp.asarray(np.concatenate([high, high, low], axis=1)))
        tables.append(jnp.asarray(np.concatenate([high, high, low], axis=0)))
    return tables


def halves(x):
    high = x.astype(jnp.bfloat16)
    return high, (x - high.astype(jnp.float32)).astype(jnp.bfloat16)


def gradient_kernel(
    offsets, counts, obj, probe, measured, left_f, right_f, left_b, right_b,
    grad, probe_grad, x3, y3, far, columns, sums,
):
    slots, length = measured.shape[0], measured.shape[1]
    modes = probe.shape[1]
    cols = obj.shape[2]
    margin = length // 2
    half = modes * length
    blocks = range(cols // length)
    for c in range(obj.shape[0]):
        for j in blocks:
            columns[c, j] = obj[c, :, j * length : (j + 1) * length]
    sums[...] = jnp.zeros_like(sums)
    probe_grad[...] = jnp.zeros_like(probe_grad)
    wide = 2 * length

    def put_x(k, part, value):
        high, low = halves(value)
        c = pl.ds(k * length, length)
        x3[pl.ds(part * length, length), c] = high
        x3[pl.ds(wide + part * length, length), c] = low
        x3[pl.ds(2 * wide + part * length, length), c] = high

    def put_y(k, part, value):
        high, low = halves(value)
        r = pl.ds(k * length, length)
        y3[r, pl.ds(part * length, length)] = high
        y3[r, pl.ds(wide + part * length, length)] = low
        y3[r, pl.ds(2 * wide + part * length, length)] = high

    def visit(s, carry):
        row = offsets[s, 0] + margin
        col = offsets[s, 1]
        shift = lax.rem(cols - col, cols)

        def cut(c):
            whole = jnp.concatenate([columns[c, j, pl.ds(row, length), :] for j in blocks], axis=1)
            return pltpu.roll(whole, shift, 1)[:, :length]

        wr, wi = cut(0), cut(1)
        energy = (wr * wr + wi * wi).reshape(-1, ENERGY_ROWS, length).sum(axis=0)
        probe_grad[0, half:, :] += energy
        probe_grad[1, half:, :] += energy
        for k in range(modes):
            pr, pi = probe[0, k], probe[1, k]
            put_x(k, 0, pr * wr - pi * wi)
            put_x(k, 1, pr * wi + pi * wr)
        left = jnp.dot(left_f[...], x3[...], preferred_element_type=jnp.float32)
        for k in range(modes):
            for part in range(2):
                put_y(k, part, left[part * length : (part + 1) * length, k * length : (k + 1) * length])
        far[...] = jnp.dot(y3[...], right_f[...], preferred_element_type=jnp.float32)
        intensity = jnp.zeros((length, length), jnp.float32)
        for k in range(modes):
            fr = far[k * length : (k + 1) * length, :length]
            fi = far[k * length : (k + 1) * length, length:]
            intensity = intensity + (fr * fr + fi * fi)
        resid = intensity - measured[s]
        for k in range(modes):
            for part in range(2):
                put_y(
                    k, part,
                    resid * far[k * length : (k + 1) * length, part * length : (part + 1) * length],
                )
        right = jnp.dot(y3[...], right_b[...], preferred_element_type=jnp.float32)
        for k in range(modes):
            for part in range(2):
                put_x(k, part, right[k * length : (k + 1) * length, part * length : (part + 1) * length])
        back = jnp.dot(left_b[...], x3[...], preferred_element_type=jnp.float32)
        gr = jnp.zeros((length, length), jnp.float32)
        gi = jnp.zeros((length, length), jnp.float32)
        wr, wi = cut(0), cut(1)
        for k in range(modes):
            pr, pi = probe[0, k], probe[1, k]
            br = back[:length, k * length : (k + 1) * length]
            bi = back[length:, k * length : (k + 1) * length]
            gr = gr + (pr * br + pi * bi)
            gi = gi + (pr * bi - pi * br)
            probe_grad[0, k * length : (k + 1) * length, :] += wr * br + wi * bi
            probe_grad[1, k * length : (k + 1) * length, :] += wr * bi - wi * br
        rest = jnp.zeros((length, cols - length), jnp.float32)
        for c, g in ((0, gr), (1, gi)):
            placed = pltpu.roll(jnp.concatenate([g, rest], axis=1), col, 1)
            for j in blocks:
                sums[c, j, pl.ds(row, length), :] += placed[:, j * length : (j + 1) * length]
        return carry

    lax.fori_loop(0, jnp.minimum(counts[0], slots), visit, 0)
    for c in range(obj.shape[0]):
        for j in blocks:
            grad[c, :, j * length : (j + 1) * length] = sums[c, j]


def greet(me, n, devices):
    barrier = pltpu.get_barrier_semaphore()

    def signal(device):
        pl.semaphore_signal(barrier, inc=1, device_id={"row": device}, device_id_type=MESH)

    pl.when(me > 0)(lambda: signal(me - 1))
    pl.when(me < n - 1)(lambda: signal(me + 1))
    for device in devices:
        signal(device)
    inside = (me > 0) & (me < n - 1)
    pl.when(inside)(lambda: pl.semaphore_wait(barrier, len(devices) + 2))
    pl.when(jnp.logical_not(inside))(lambda: pl.semaphore_wait(barrier, len(devices) + 1))


def remote(src, dst, send, recv, device):
    return pltpu.make_async_remote_copy(
        src_ref=src, dst_ref=dst, send_sem=send, recv_sem=recv,
        device_id={"row": device}, device_id_type=MESH,
    )


def exchange(me, n, array, rows_up, rows_down, from_up, from_down, sems):
    up = remote(array.at[:, rows_up], from_down, sems.at[0], sems.at[1], me - 1)
    down = remote(array.at[:, rows_down], from_up, sems.at[2], sems.at[3], me + 1)

    def start():
        pl.when(me > 0)(up.start)
        pl.when(me < n - 1)(down.start)

    def wait():
        @pl.when(me > 0)
        def _():
            up.wait_send()
            down.wait_recv()

        @pl.when(me < n - 1)
        def _():
            down.wait_send()
            up.wait_recv()

    return start, wait


def halo_kernel(n, tile, padded, from_up, from_down, sems):
    me = lax.axis_index("row")
    rows = tile.shape[1]
    margin = from_up.shape[1]
    greet(me, n, [])
    start, wait = exchange(
        me, n, tile, pl.ds(0, margin), pl.ds(rows - margin, margin), from_up, from_down, sems
    )
    start()
    padded[:, margin : margin + rows] = tile[...]

    @pl.when(me == 0)
    def _():
        padded[:, :margin] = jnp.zeros_like(from_up)

    @pl.when(me == n - 1)
    def _():
        padded[:, margin + rows :] = jnp.zeros_like(from_down)

    wait()

    @pl.when(me > 0)
    def _():
        padded[:, :margin] = from_up[...]

    @pl.when(me < n - 1)
    def _():
        padded[:, margin + rows :] = from_down[...]


def update_kernel(
    n, final, modes, obj, grad, probe, probe_grad, new_obj, new_probe,
    from_up, from_down, r1, t2, r2, t3, r3, fresh, edge_sems, pair_sems,
    out3, in3, gout3, gin3, gout2, gin2, gout1, gin1,
):
    me = lax.axis_index("row")
    length = probe.shape[1]
    margin = length // 2
    padded_rows = obj.shape[1]
    edge = from_up.shape[1]
    peers = t3.shape[0]
    rows = t3.shape[1] - ENERGY_ROWS
    half, quarter = probe.shape[0] // 2, probe.shape[0] // 4
    core = me % 2
    second = (me // 2) % 2
    rank = me // 4
    mate = me + 1 - 2 * core
    other = me + 2 - 4 * second
    ranks = [(rank + d) % peers for d in range(1, peers)]
    greet(me, n, [mate, other] + [p * 4 + me % 4 for p in ranks])
    one = remote(probe_grad.at[1 - core], r1, pair_sems.at[0], pair_sems.at[1], mate)
    one.start()
    rows_up, rows_down = pl.ds(0, edge), pl.ds(padded_rows - edge, edge)
    start, wait = exchange(me, n, grad, rows_up, rows_down, from_up, from_down, edge_sems)
    start()
    power = jnp.zeros((length, length), jnp.float32)
    for k in range(2 * modes):
        p = probe[k * length : (k + 1) * length, :]
        power = power + p * p
    step = object_rate / jnp.max(power, axis=(0, 1), keepdims=True)

    @pl.when(me == 0)
    def _():
        from_up[...] = jnp.zeros_like(from_up)

    @pl.when(me == n - 1)
    def _():
        from_down[...] = jnp.zeros_like(from_down)

    one.wait()
    for b in range(2):
        t2[b, :quarter] = (
            probe_grad[core, b * quarter : (b + 1) * quarter] + r1[b * quarter : (b + 1) * quarter]
        )
        t2[b, quarter:] = probe_grad[core, half:] + r1[half:]
    two = remote(t2.at[1 - second], r2, pair_sems.at[2], pair_sems.at[3], other)
    two.start()

    base = margin if final else 0
    inner = slice(base + edge, padded_rows - base - edge)

    def out(s):
        return slice(s.start - base, s.stop - base)

    new_obj[:, out(inner)] = obj[:, inner] - step * grad[:, inner]
    wait()
    top = slice(base, base + edge)
    low = slice(padded_rows - base - edge, padded_rows - base)
    new_obj[:, out(top)] = obj[:, top] - step * (grad[:, top] + from_up[...])
    new_obj[:, out(low)] = obj[:, low] - step * (grad[:, low] + from_down[...])
    if not final:
        @pl.when(me == 0)
        def _():
            new_obj[:, :margin] = jnp.zeros((2, margin, obj.shape[2]), jnp.float32)

        @pl.when(me == n - 1)
        def _():
            new_obj[:, padded_rows - margin :] = jnp.zeros((2, margin, obj.shape[2]), jnp.float32)

    two.wait()
    for p in range(peers):
        t3[p, :rows] = t2[second, p * rows : (p + 1) * rows] + r2[p * rows : (p + 1) * rows]
        t3[p, rows:] = t2[second, quarter:] + r2[quarter:]
    sends = []
    for p in ranks:
        sends.append(remote(t3.at[p], r3.at[rank], out3.at[p], in3.at[rank], p * 4 + me % 4))
        sends[-1].start()
    share = t3[rank]
    for p in ranks:
        remote(t3.at[p], r3.at[p], out3.at[p], in3.at[p], p * 4 + me % 4).wait_recv()
        share = share + r3[p]
    energy = jnp.sum(share[rows:], axis=(0, 1), keepdims=True)

    def region(c, b, p):
        return pl.ds(pl.multiple_of(c * half + b * quarter + p * rows, rows), rows)

    own = region(core, second, rank)
    fresh[own, :] = probe[own, :] - probe_rate * length * length / energy * share[:rows]

    def to_rank(p, q):
        part = fresh.at[region(core, second, q)]
        return remote(part, part, gout3.at[p], gin3.at[q], p * 4 + me % 4)

    def to_other(b, p):
        part = fresh.at[region(core, b, p)]
        return remote(part, part, gout2.at[p], gin2.at[p], other)

    def to_mate(c, b, p):
        part = fresh.at[region(c, b, p)]
        return remote(part, part, gout1.at[b * peers + p], gin1.at[b * peers + p], mate)

    def pass_on(copy):
        copy.start()
        sends.append(copy)

    for p in ranks:
        pass_on(to_rank(p, rank))
    pass_on(to_other(second, rank))
    pass_on(to_mate(core, second, rank))
    for p in ranks:
        to_rank(p, p).wait_recv()
        pass_on(to_other(second, p))
        pass_on(to_mate(core, second, p))
    for p in [rank] + ranks:
        to_other(1 - second, p).wait_recv()
        pass_on(to_mate(core, 1 - second, p))
    for p in [rank] + ranks:
        to_mate(1 - core, second, p).wait_recv()
    for p in [rank] + ranks:
        to_mate(1 - core, 1 - second, p).wait_recv()
    new_probe[...] = fresh[...]
    for copy in sends:
        copy.wait_send()


def body(object_tile, probe_modes, measured, offsets, counts):
    n = lax.axis_size("row")
    parts, tile_rows, cols = object_tile.shape
    modes, length = probe_modes.shape[1], probe_modes.shape[2]
    margin = length // 2
    padded_rows = tile_rows + 2 * margin
    flat = 2 * modes * length
    half, quarter = flat // 2, flat // 4
    peers = n // 4
    rows = quarter // peers
    f32 = jnp.float32
    dma = pltpu.SemaphoreType.DMA
    padded_shape = jax.ShapeDtypeStruct((parts, padded_rows, cols), f32)
    tables = dft_tables(length)

    padded = pl.pallas_call(
        functools.partial(halo_kernel, n),
        name="halo",
        out_shape=padded_shape,
        in_specs=[VMEM],
        out_specs=VMEM,
        scratch_shapes=[pltpu.VMEM((parts, margin, cols), f32)] * 2 + [dma((4,))],
        compiler_params=pltpu.CompilerParams(collective_id=0, has_side_effects=True),
    )(object_tile)

    gradient = pl.pallas_call(
        gradient_kernel,
        name="gradient",
        out_shape=[padded_shape, jax.ShapeDtypeStruct((2, half + ENERGY_ROWS, length), f32)],
        in_specs=[SMEM, SMEM] + [VMEM] * 7,
        out_specs=[VMEM, VMEM],
        scratch_shapes=[
            pltpu.VMEM((6 * length, modes * length), jnp.bfloat16),
            pltpu.VMEM((modes * length, 6 * length), jnp.bfloat16),
            pltpu.VMEM((modes * length, 2 * length), f32),
        ]
        + [pltpu.VMEM((parts, cols // length, padded_rows, length), f32)] * 2,
    )

    probe_now = probe_modes
    for sweep in range(ITERS):
        final = sweep == ITERS - 1
        edge = margin if final else 2 * margin
        grad, probe_grad = gradient(
            offsets, counts, padded, probe_now, measured, tables[0], tables[3], tables[2], tables[1]
        )
        padded, fresh = pl.pallas_call(
            functools.partial(update_kernel, n, final, modes),
            name="update_last" if final else "update",
            out_shape=[
                jax.ShapeDtypeStruct((parts, tile_rows if final else padded_rows, cols), f32),
                jax.ShapeDtypeStruct((flat, length), f32),
            ],
            in_specs=[VMEM] * 4,
            out_specs=[VMEM] * 2,
            scratch_shapes=[
                pltpu.VMEM((parts, edge, cols), f32),
                pltpu.VMEM((parts, edge, cols), f32),
                pltpu.VMEM((half + ENERGY_ROWS, length), f32),
                pltpu.VMEM((2, quarter + ENERGY_ROWS, length), f32),
                pltpu.VMEM((quarter + ENERGY_ROWS, length), f32),
                pltpu.VMEM((peers, rows + ENERGY_ROWS, length), f32),
                pltpu.VMEM((peers, rows + ENERGY_ROWS, length), f32),
                pltpu.VMEM((flat, length), f32),
                dma((4,)),
                dma((4,)),
                dma((peers,)), dma((peers,)), dma((peers,)), dma((peers,)),
                dma((peers,)), dma((peers,)), dma((2 * peers,)), dma((2 * peers,)),
            ],
            compiler_params=pltpu.CompilerParams(
                collective_id=1 + sweep, has_side_effects=True
            ),
        )(padded, grad, probe_now.reshape(flat, length), probe_grad)
        probe_now = fresh.reshape(probe_modes.shape)
    return (padded, probe_now)


def solution(mesh):
    return jax.shard_map(
        body,
        mesh=mesh,
        in_specs=(
            P(None, ("parts", "row"), None),
            P(),
            P(("parts", "row"), None, None),
            P(("parts", "row"), None),
            P(("parts", "row")),
        ),
        out_specs=(P(None, ("parts", "row"), None), P("parts", None, None, None)),
        check_vma=False,
    )
```

```python
import functools
import math

import jax
import jax.numpy as jnp
import numpy as np
from jax import lax
from jax.experimental import pallas as pl
from jax.experimental.pallas import tpu as pltpu
from jax.sharding import PartitionSpec as P

ITERS = 2
object_rate = 0.2
probe_rate = 0.5
ENERGY_ROWS = 8
VMEM = pl.BlockSpec(memory_space=pltpu.VMEM)
ANY = pl.BlockSpec(memory_space=pl.ANY)
SMEM = pl.BlockSpec(memory_space=pltpu.SMEM)
MESH = pl.DeviceIdType.MESH


def dft_tables(length):
    index = np.arange(length)
    phase = 2.0 * math.pi / length * (index[:, None] * index[None, :] % length)
    cosine = np.cos(phase) / math.sqrt(length)
    sine = -np.sin(phase) / math.sqrt(length)
    forward = np.block([[cosine, -sine], [sine, cosine]]).astype(np.float32)
    backward = np.block([[cosine, sine], [-sine, cosine]]).astype(np.float32)
    tables = []
    for table in (forward, backward):
        high = table.astype(jnp.bfloat16)
        low = (table - high.astype(np.float32)).astype(jnp.bfloat16)
        tables.append(jnp.asarray(np.concatenate([high, high, low], axis=1)))
        tables.append(jnp.asarray(np.concatenate([high, high, low], axis=0)))
    return tables


def halves(x):
    high = x.astype(jnp.bfloat16)
    return high, (x - high.astype(jnp.float32)).astype(jnp.bfloat16)


def gradient_kernel(
    offsets, counts, obj, probe, measured, left_f, right_f, left_b, right_b,
    grad, probe_grad, x3, y3, far, columns, sums,
):
    slots, length = measured.shape[0], measured.shape[1]
    modes = probe.shape[1]
    cols = obj.shape[2]
    margin = length // 2
    half = modes * length
    blocks = range(cols // length)
    for c in range(obj.shape[0]):
        for j in blocks:
            columns[c, j] = obj[c, :, j * length : (j + 1) * length]
    sums[...] = jnp.zeros_like(sums)
    probe_grad[...] = jnp.zeros_like(probe_grad)
    wide = 2 * length

    def put_x(k, part, value):
        high, low = halves(value)
        c = pl.ds(k * length, length)
        x3[pl.ds(part * length, length), c] = high
        x3[pl.ds(wide + part * length, length), c] = low
        x3[pl.ds(2 * wide + part * length, length), c] = high

    def put_y(k, part, value):
        high, low = halves(value)
        r = pl.ds(k * length, length)
        y3[r, pl.ds(part * length, length)] = high
        y3[r, pl.ds(wide + part * length, length)] = low
        y3[r, pl.ds(2 * wide + part * length, length)] = high

    def visit(s, carry):
        row = offsets[0, s] + margin
        col = offsets[1, s]
        shift = lax.rem(cols - col, cols)

        def cut(c):
            whole = jnp.concatenate([columns[c, j, pl.ds(row, length), :] for j in blocks], axis=1)
            return pltpu.roll(whole, shift, 1)[:, :length]

        wr, wi = cut(0), cut(1)
        energy = (wr * wr + wi * wi).reshape(-1, ENERGY_ROWS, length).sum(axis=0)
        probe_grad[0, half:, :] += energy
        probe_grad[1, half:, :] += energy
        for k in range(modes):
            pr, pi = probe[0, k], probe[1, k]
            put_x(k, 0, pr * wr - pi * wi)
            put_x(k, 1, pr * wi + pi * wr)
        left = jnp.dot(left_f[...], x3[...], preferred_element_type=jnp.float32)
        for k in range(modes):
            for part in range(2):
                put_y(k, part, left[part * length : (part + 1) * length, k * length : (k + 1) * length])
        far[...] = jnp.dot(y3[...], right_f[...], preferred_element_type=jnp.float32)
        intensity = jnp.zeros((length, length), jnp.float32)
        for k in range(modes):
            fr = far[k * length : (k + 1) * length, :length]
            fi = far[k * length : (k + 1) * length, length:]
            intensity = intensity + (fr * fr + fi * fi)
        resid = intensity - measured[s]
        for k in range(modes):
            for part in range(2):
                put_y(
                    k, part,
                    resid * far[k * length : (k + 1) * length, part * length : (part + 1) * length],
                )
        right = jnp.dot(y3[...], right_b[...], preferred_element_type=jnp.float32)
        for k in range(modes):
            for part in range(2):
                put_x(k, part, right[k * length : (k + 1) * length, part * length : (part + 1) * length])
        back = jnp.dot(left_b[...], x3[...], preferred_element_type=jnp.float32)
        gr = jnp.zeros((length, length), jnp.float32)
        gi = jnp.zeros((length, length), jnp.float32)
        wr, wi = cut(0), cut(1)
        for k in range(modes):
            pr, pi = probe[0, k], probe[1, k]
            br = back[:length, k * length : (k + 1) * length]
            bi = back[length:, k * length : (k + 1) * length]
            gr = gr + (pr * br + pi * bi)
            gi = gi + (pr * bi - pi * br)
            probe_grad[0, k * length : (k + 1) * length, :] += wr * br + wi * bi
            probe_grad[1, k * length : (k + 1) * length, :] += wr * bi - wi * br
        rest = jnp.zeros((length, cols - length), jnp.float32)
        for c, g in ((0, gr), (1, gi)):
            placed = pltpu.roll(jnp.concatenate([g, rest], axis=1), col, 1)
            for j in blocks:
                sums[c, j, pl.ds(row, length), :] += placed[:, j * length : (j + 1) * length]
        return carry

    lax.fori_loop(0, jnp.minimum(counts[0], slots), visit, 0)
    for c in range(obj.shape[0]):
        for j in blocks:
            grad[c, :, j * length : (j + 1) * length] = sums[c, j]


def greet(me, n, devices):
    barrier = pltpu.get_barrier_semaphore()

    def signal(device):
        pl.semaphore_signal(barrier, inc=1, device_id={"row": device}, device_id_type=MESH)

    pl.when(me > 0)(lambda: signal(me - 1))
    pl.when(me < n - 1)(lambda: signal(me + 1))
    for device in devices:
        signal(device)
    inside = (me > 0) & (me < n - 1)
    pl.when(inside)(lambda: pl.semaphore_wait(barrier, len(devices) + 2))
    pl.when(jnp.logical_not(inside))(lambda: pl.semaphore_wait(barrier, len(devices) + 1))


def remote(src, dst, send, recv, device):
    return pltpu.make_async_remote_copy(
        src_ref=src, dst_ref=dst, send_sem=send, recv_sem=recv,
        device_id={"row": device}, device_id_type=MESH,
    )


def exchange(me, n, array, rows_up, rows_down, from_up, from_down, sems):
    up = remote(array.at[:, rows_up], from_down, sems.at[0], sems.at[1], me - 1)
    down = remote(array.at[:, rows_down], from_up, sems.at[2], sems.at[3], me + 1)

    def start():
        pl.when(me > 0)(up.start)
        pl.when(me < n - 1)(down.start)

    def wait():
        @pl.when(me > 0)
        def _():
            up.wait_send()
            down.wait_recv()

        @pl.when(me < n - 1)
        def _():
            down.wait_send()
            up.wait_recv()

    return start, wait


def halo_kernel(n, tile, padded, from_up, from_down, sems):
    me = lax.axis_index("row")
    rows = tile.shape[1]
    margin = from_up.shape[1]
    greet(me, n, [])
    start, wait = exchange(
        me, n, tile, pl.ds(0, margin), pl.ds(rows - margin, margin), from_up, from_down, sems
    )
    start()
    padded[:, margin : margin + rows] = tile[...]

    @pl.when(me == 0)
    def _():
        padded[:, :margin] = jnp.zeros_like(from_up)

    @pl.when(me == n - 1)
    def _():
        padded[:, margin + rows :] = jnp.zeros_like(from_down)

    wait()

    @pl.when(me > 0)
    def _():
        padded[:, :margin] = from_up[...]

    @pl.when(me < n - 1)
    def _():
        padded[:, margin + rows :] = from_down[...]


def update_kernel(
    n, final, modes, obj_in, grad_in, probe_in, probe_grad, new_obj, new_probe,
    from_up, from_down, obj, grad, made, probe, r1, t2, r2, t3, r3, fresh,
    local_sems, edge_sems, pair_sems, out2, in2,
    out3, in3, gout3, gin3, gout2, gin2, gout1, gin1,
):
    me = lax.axis_index("row")
    length = probe.shape[1]
    margin = length // 2
    padded_rows = obj.shape[1]
    edge = from_up.shape[1]
    peers = t3.shape[0]
    rows = t3.shape[1] - ENERGY_ROWS
    half, quarter = probe.shape[0] // 2, probe.shape[0] // 4
    core = me % 2
    second = (me // 2) % 2
    rank = me // 4
    mate = me + 1 - 2 * core
    other = me + 2 - 4 * second
    ranks = [(rank + d) % peers for d in range(1, peers)]
    loads = [
        pltpu.make_async_copy(src, dst, local_sems.at[i])
        for i, (src, dst) in enumerate(((probe_in, probe), (obj_in, obj), (grad_in, grad)))
    ]
    for load in loads:
        load.start()
    greet(me, n, [mate, other] + [p * 4 + me % 4 for p in ranks])
    one = remote(probe_grad.at[1 - core], r1, pair_sems.at[0], pair_sems.at[1], mate)
    one.start()

    @pl.when(me == 0)
    def _():
        from_up[...] = jnp.zeros_like(from_up)

    @pl.when(me == n - 1)
    def _():
        from_down[...] = jnp.zeros_like(from_down)

    one.wait_recv()

    def add_pair(b, p):
        part = pl.ds(pl.multiple_of(b * quarter + p * rows, rows), rows)
        t2[b, p, :rows] = probe_grad[core, part] + r1[part]
        t2[b, p, rows:] = probe_grad[core, half:] + r1[half:]

    sends = [one]

    def pass_on(copy):
        copy.start()
        sends.append(copy)

    def to_second(p):
        return remote(t2.at[1 - second, p], r2.at[p], out2.at[p], in2.at[p], other)

    for p in ranks + [rank]:
        add_pair(1 - second, p)
        pass_on(to_second(p))
    start, wait = exchange(
        me, n, grad_in, pl.ds(0, edge), pl.ds(padded_rows - edge, edge), from_up, from_down, edge_sems
    )
    start()
    for p in ranks + [rank]:
        add_pair(second, p)
    for p in ranks + [rank]:
        to_second(p).wait_recv()
        t3[p] = t2[second, p] + r2[p]
        if p is not rank:
            pass_on(remote(t3.at[p], r3.at[rank], out3.at[p], in3.at[rank], p * 4 + me % 4))

    loads[0].wait()
    power = jnp.zeros((length, length), jnp.float32)
    for k in range(2 * modes):
        p = probe[k * length : (k + 1) * length, :]
        power = power + p * p
    step = object_rate / jnp.max(power, axis=(0, 1), keepdims=True)
    loads[1].wait()
    loads[2].wait()
    base = margin if final else 0

    def out(s):
        return slice(s.start - base, s.stop - base)

    inner = slice(base + edge, padded_rows - base - edge)
    top = slice(base, base + edge)
    low = slice(padded_rows - base - edge, padded_rows - base)
    made[:, out(inner)] = obj[:, inner] - step * grad[:, inner]

    share = t3[rank]
    for p in ranks:
        remote(t3.at[p], r3.at[p], out3.at[p], in3.at[p], p * 4 + me % 4).wait_recv()
        share = share + r3[p]
    energy = jnp.sum(share[rows:], axis=(0, 1), keepdims=True)

    def region(c, b, p):
        return pl.ds(pl.multiple_of(c * half + b * quarter + p * rows, rows), rows)

    own = region(core, second, rank)
    fresh[own, :] = probe[own, :] - probe_rate * length * length / energy * share[:rows]

    def to_rank(p, q):
        part = fresh.at[region(core, second, q)]
        return remote(part, part, gout3.at[p], gin3.at[q], p * 4 + me % 4)

    def to_other(b, p):
        part = fresh.at[region(core, b, p)]
        return remote(part, part, gout2.at[p], gin2.at[p], other)

    def to_mate(c, b, p):
        part = fresh.at[region(c, b, p)]
        return remote(part, part, gout1.at[b * peers + p], gin1.at[b * peers + p], mate)

    for p in ranks:
        pass_on(to_rank(p, rank))
    pass_on(to_other(second, rank))
    pass_on(to_mate(core, second, rank))

    wait()
    made[:, out(top)] = obj[:, top] - step * (grad[:, top] + from_up[...])
    made[:, out(low)] = obj[:, low] - step * (grad[:, low] + from_down[...])
    if not final:
        @pl.when(me == 0)
        def _():
            made[:, :margin] = jnp.zeros((2, margin, obj.shape[2]), jnp.float32)

        @pl.when(me == n - 1)
        def _():
            made[:, padded_rows - margin :] = jnp.zeros((2, margin, obj.shape[2]), jnp.float32)

    store = pltpu.make_async_copy(made, new_obj, local_sems.at[1])
    store.start()
    for p in ranks:
        to_rank(p, p).wait_recv()
        pass_on(to_other(second, p))
        pass_on(to_mate(core, second, p))
    for p in [rank] + ranks:
        to_other(1 - second, p).wait_recv()
        pass_on(to_mate(core, 1 - second, p))
    for p in [rank] + ranks:
        to_mate(1 - core, second, p).wait_recv()
    for p in [rank] + ranks:
        to_mate(1 - core, 1 - second, p).wait_recv()
    result = pltpu.make_async_copy(fresh, new_probe, local_sems.at[0])
    result.start()
    for copy in sends:
        copy.wait_send()
    store.wait()
    result.wait()


def body(object_tile, probe_modes, measured, offsets, counts):
    n = lax.axis_size("row")
    parts, tile_rows, cols = object_tile.shape
    modes, length = probe_modes.shape[1], probe_modes.shape[2]
    margin = length // 2
    padded_rows = tile_rows + 2 * margin
    flat = 2 * modes * length
    half, quarter = flat // 2, flat // 4
    peers = n // 4
    rows = quarter // peers
    f32 = jnp.float32
    dma = pltpu.SemaphoreType.DMA
    padded_shape = jax.ShapeDtypeStruct((parts, padded_rows, cols), f32)
    tables = dft_tables(length)

    padded = pl.pallas_call(
        functools.partial(halo_kernel, n),
        name="halo",
        out_shape=padded_shape,
        in_specs=[VMEM],
        out_specs=VMEM,
        scratch_shapes=[pltpu.VMEM((parts, margin, cols), f32)] * 2 + [dma((4,))],
        compiler_params=pltpu.CompilerParams(collective_id=0, has_side_effects=True),
    )(object_tile)

    gradient = pl.pallas_call(
        gradient_kernel,
        name="gradient",
        out_shape=[padded_shape, jax.ShapeDtypeStruct((2, half + ENERGY_ROWS, length), f32)],
        in_specs=[SMEM, SMEM] + [VMEM] * 7,
        out_specs=[VMEM, VMEM],
        scratch_shapes=[
            pltpu.VMEM((6 * length, modes * length), jnp.bfloat16),
            pltpu.VMEM((modes * length, 6 * length), jnp.bfloat16),
            pltpu.VMEM((modes * length, 2 * length), f32),
        ]
        + [pltpu.VMEM((parts, cols // length, padded_rows, length), f32)] * 2,
    )

    probe_now = probe_modes
    for sweep in range(ITERS):
        final = sweep == ITERS - 1
        edge = margin if final else 2 * margin
        grad, probe_grad = gradient(
            offsets.T, counts, padded, probe_now, measured, tables[0], tables[3], tables[2], tables[1]
        )
        padded, fresh = pl.pallas_call(
            functools.partial(update_kernel, n, final, modes),
            name="update_last" if final else "update",
            out_shape=[
                jax.ShapeDtypeStruct((parts, tile_rows if final else padded_rows, cols), f32),
                jax.ShapeDtypeStruct((flat, length), f32),
            ],
            in_specs=[ANY] * 3 + [VMEM],
            out_specs=[ANY] * 2,
            scratch_shapes=[
                pltpu.VMEM((parts, edge, cols), f32),
                pltpu.VMEM((parts, edge, cols), f32),
                pltpu.VMEM((parts, padded_rows, cols), f32),
                pltpu.VMEM((parts, padded_rows, cols), f32),
                pltpu.VMEM((parts, tile_rows if final else padded_rows, cols), f32),
                pltpu.VMEM((flat, length), f32),
                pltpu.VMEM((half + ENERGY_ROWS, length), f32),
                pltpu.VMEM((2, peers, rows + ENERGY_ROWS, length), f32),
                pltpu.VMEM((peers, rows + ENERGY_ROWS, length), f32),
                pltpu.VMEM((peers, rows + ENERGY_ROWS, length), f32),
                pltpu.VMEM((peers, rows + ENERGY_ROWS, length), f32),
                pltpu.VMEM((flat, length), f32),
                dma((3,)),
                dma((4,)),
                dma((2,)),
                dma((peers,)), dma((peers,)),
                dma((peers,)), dma((peers,)), dma((peers,)), dma((peers,)),
                dma((peers,)), dma((peers,)), dma((2 * peers,)), dma((2 * peers,)),
            ],
            compiler_params=pltpu.CompilerParams(
                collective_id=1 + sweep, has_side_effects=True
            ),
        )(padded, grad, probe_now.reshape(flat, length), probe_grad)
        probe_now = fresh.reshape(probe_modes.shape)
    return (padded, probe_now)


def solution(mesh):
    return jax.shard_map(
        body,
        mesh=mesh,
        in_specs=(
            P(None, ("parts", "row"), None),
            P(),
            P(("parts", "row"), None, None),
            P(("parts", "row"), None),
            P(("parts", "row")),
        ),
        out_specs=(P(None, ("parts", "row"), None), P("parts", None, None, None)),
        check_vma=False,
    )
```

```python
import functools
import math

import jax
import jax.numpy as jnp
import numpy as np
from jax import lax
from jax.experimental import pallas as pl
from jax.experimental.pallas import tpu as pltpu
from jax.sharding import PartitionSpec as P

ITERS = 2
object_rate = 0.2
probe_rate = 0.5
ENERGY_ROWS = 8
VMEM = pl.BlockSpec(memory_space=pltpu.VMEM)
ANY = pl.BlockSpec(memory_space=pl.ANY)
SMEM = pl.BlockSpec(memory_space=pltpu.SMEM)
MESH = pl.DeviceIdType.MESH


def dft_tables(length):
    index = np.arange(length)
    phase = 2.0 * math.pi / length * (index[:, None] * index[None, :] % length)
    cosine = np.cos(phase) / math.sqrt(length)
    sine = -np.sin(phase) / math.sqrt(length)
    forward = np.block([[cosine, -sine], [sine, cosine]]).astype(np.float32)
    backward = np.block([[cosine, sine], [-sine, cosine]]).astype(np.float32)
    tables = []
    for table in (forward, backward):
        high = table.astype(jnp.bfloat16)
        low = (table - high.astype(np.float32)).astype(jnp.bfloat16)
        tables.append(jnp.asarray(np.concatenate([high, high, low], axis=1)))
        tables.append(jnp.asarray(np.concatenate([high, high, low], axis=0)))
    return tables


def halves(x):
    high = x.astype(jnp.bfloat16)
    return high, (x - high.astype(jnp.float32)).astype(jnp.bfloat16)


def gradient_kernel(
    offsets, counts, obj, probe, measured_in, left_f_in, right_f_in, left_b_in, right_b_in,
    grad, probe_grad, x3, y3, far, columns, sums,
    measured, left_f, right_f, left_b, right_b, load_sems,
):
    slots, length = measured.shape[0], measured.shape[1]
    modes = probe.shape[1]
    cols = obj.shape[2]
    margin = length // 2
    half = modes * length
    pairs = (
        (left_f_in, left_f), (right_f_in, right_f), (measured_in, measured),
        (right_b_in, right_b), (left_b_in, left_b),
    )
    loads = [pltpu.make_async_copy(a, b, load_sems.at[i]) for i, (a, b) in enumerate(pairs)]
    for load in loads:
        load.start()
    blocks = range(cols // length)
    for c in range(obj.shape[0]):
        for j in blocks:
            columns[c, j] = obj[c, :, j * length : (j + 1) * length]
    sums[...] = jnp.zeros_like(sums)
    probe_grad[...] = jnp.zeros_like(probe_grad)
    wide = 2 * length
    for load in loads:
        load.wait()

    def put_x(k, part, value):
        high, low = halves(value)
        c = pl.ds(k * length, length)
        x3[pl.ds(part * length, length), c] = high
        x3[pl.ds(wide + part * length, length), c] = low
        x3[pl.ds(2 * wide + part * length, length), c] = high

    def put_y(k, part, value):
        high, low = halves(value)
        r = pl.ds(k * length, length)
        y3[r, pl.ds(part * length, length)] = high
        y3[r, pl.ds(wide + part * length, length)] = low
        y3[r, pl.ds(2 * wide + part * length, length)] = high

    def visit(s, carry):
        row = offsets[0, s] + margin
        col = offsets[1, s]
        shift = lax.rem(cols - col, cols)

        def cut(c):
            whole = jnp.concatenate([columns[c, j, pl.ds(row, length), :] for j in blocks], axis=1)
            return pltpu.roll(whole, shift, 1)[:, :length]

        wr, wi = cut(0), cut(1)
        energy = (wr * wr + wi * wi).reshape(-1, ENERGY_ROWS, length).sum(axis=0)
        probe_grad[0, half:, :] += energy
        probe_grad[1, half:, :] += energy
        for k in range(modes):
            pr, pi = probe[0, k], probe[1, k]
            put_x(k, 0, pr * wr - pi * wi)
            put_x(k, 1, pr * wi + pi * wr)
        left = jnp.dot(left_f[...], x3[...], preferred_element_type=jnp.float32)
        for k in range(modes):
            for part in range(2):
                put_y(k, part, left[part * length : (part + 1) * length, k * length : (k + 1) * length])
        far[...] = jnp.dot(y3[...], right_f[...], preferred_element_type=jnp.float32)
        intensity = jnp.zeros((length, length), jnp.float32)
        for k in range(modes):
            fr = far[k * length : (k + 1) * length, :length]
            fi = far[k * length : (k + 1) * length, length:]
            intensity = intensity + (fr * fr + fi * fi)
        resid = intensity - measured[s]
        for k in range(modes):
            for part in range(2):
                put_y(
                    k, part,
                    resid * far[k * length : (k + 1) * length, part * length : (part + 1) * length],
                )
        right = jnp.dot(y3[...], right_b[...], preferred_element_type=jnp.float32)
        for k in range(modes):
            for part in range(2):
                put_x(k, part, right[k * length : (k + 1) * length, part * length : (part + 1) * length])
        back = jnp.dot(left_b[...], x3[...], preferred_element_type=jnp.float32)
        gr = jnp.zeros((length, length), jnp.float32)
        gi = jnp.zeros((length, length), jnp.float32)
        wr, wi = cut(0), cut(1)
        for k in range(modes):
            pr, pi = probe[0, k], probe[1, k]
            br = back[:length, k * length : (k + 1) * length]
            bi = back[length:, k * length : (k + 1) * length]
            gr = gr + (pr * br + pi * bi)
            gi = gi + (pr * bi - pi * br)
            probe_grad[0, k * length : (k + 1) * length, :] += wr * br + wi * bi
            probe_grad[1, k * length : (k + 1) * length, :] += wr * bi - wi * br
        rest = jnp.zeros((length, cols - length), jnp.float32)
        for c, g in ((0, gr), (1, gi)):
            placed = pltpu.roll(jnp.concatenate([g, rest], axis=1), col, 1)
            for j in blocks:
                sums[c, j, pl.ds(row, length), :] += placed[:, j * length : (j + 1) * length]
        return carry

    lax.fori_loop(0, jnp.minimum(counts[0], slots), visit, 0)
    for c in range(obj.shape[0]):
        for j in blocks:
            grad[c, :, j * length : (j + 1) * length] = sums[c, j]


def greet(me, n, devices):
    barrier = pltpu.get_barrier_semaphore()

    def signal(device):
        pl.semaphore_signal(barrier, inc=1, device_id={"row": device}, device_id_type=MESH)

    pl.when(me > 0)(lambda: signal(me - 1))
    pl.when(me < n - 1)(lambda: signal(me + 1))
    for device in devices:
        signal(device)
    inside = (me > 0) & (me < n - 1)
    pl.when(inside)(lambda: pl.semaphore_wait(barrier, len(devices) + 2))
    pl.when(jnp.logical_not(inside))(lambda: pl.semaphore_wait(barrier, len(devices) + 1))


def remote(src, dst, send, recv, device):
    return pltpu.make_async_remote_copy(
        src_ref=src, dst_ref=dst, send_sem=send, recv_sem=recv,
        device_id={"row": device}, device_id_type=MESH,
    )


def exchange(me, n, array, rows_up, rows_down, from_up, from_down, sems):
    up = remote(array.at[:, rows_up], from_down, sems.at[0], sems.at[1], me - 1)
    down = remote(array.at[:, rows_down], from_up, sems.at[2], sems.at[3], me + 1)

    def start():
        pl.when(me > 0)(up.start)
        pl.when(me < n - 1)(down.start)

    def wait():
        @pl.when(me > 0)
        def _():
            up.wait_send()
            down.wait_recv()

        @pl.when(me < n - 1)
        def _():
            down.wait_send()
            up.wait_recv()

    return start, wait


def halo_kernel(n, tile, padded, from_up, from_down, sems):
    me = lax.axis_index("row")
    rows = tile.shape[1]
    margin = from_up.shape[1]
    greet(me, n, [])
    start, wait = exchange(
        me, n, tile, pl.ds(0, margin), pl.ds(rows - margin, margin), from_up, from_down, sems
    )
    start()
    padded[:, margin : margin + rows] = tile[...]

    @pl.when(me == 0)
    def _():
        padded[:, :margin] = jnp.zeros_like(from_up)

    @pl.when(me == n - 1)
    def _():
        padded[:, margin + rows :] = jnp.zeros_like(from_down)

    wait()

    @pl.when(me > 0)
    def _():
        padded[:, :margin] = from_up[...]

    @pl.when(me < n - 1)
    def _():
        padded[:, margin + rows :] = from_down[...]


def update_kernel(
    n, final, modes, obj_in, grad_in, probe_in, probe_grad, new_obj, new_probe,
    from_up, from_down, obj, grad, made, probe, r1, t2, r2, t3, r3, fresh,
    local_sems, edge_sems, pair_sems, out2, in2,
    out3, in3, gout3, gin3, gout2, gin2, gout1, gin1,
):
    me = lax.axis_index("row")
    length = probe.shape[1]
    margin = length // 2
    padded_rows = obj.shape[1]
    edge = from_up.shape[1]
    peers = t3.shape[0]
    rows = t3.shape[1] - ENERGY_ROWS
    half, quarter = probe.shape[0] // 2, probe.shape[0] // 4
    core = me % 2
    second = (me // 2) % 2
    rank = me // 4
    mate = me + 1 - 2 * core
    other = me + 2 - 4 * second
    ranks = [(rank + d) % peers for d in range(1, peers)]
    loads = [
        pltpu.make_async_copy(src, dst, local_sems.at[i])
        for i, (src, dst) in enumerate(((probe_in, probe), (obj_in, obj), (grad_in, grad)))
    ]
    for load in loads:
        load.start()
    greet(me, n, [mate, other] + [p * 4 + me % 4 for p in ranks])
    one = remote(probe_grad.at[1 - core], r1, pair_sems.at[0], pair_sems.at[1], mate)
    one.start()

    @pl.when(me == 0)
    def _():
        from_up[...] = jnp.zeros_like(from_up)

    @pl.when(me == n - 1)
    def _():
        from_down[...] = jnp.zeros_like(from_down)

    one.wait_recv()

    def add_pair(b, p):
        part = pl.ds(pl.multiple_of(b * quarter + p * rows, rows), rows)
        t2[b, p, :rows] = probe_grad[core, part] + r1[part]
        t2[b, p, rows:] = probe_grad[core, half:] + r1[half:]

    sends = [one]

    def pass_on(copy):
        copy.start()
        sends.append(copy)

    def to_second(p):
        return remote(t2.at[1 - second, p], r2.at[p], out2.at[p], in2.at[p], other)

    for p in ranks + [rank]:
        add_pair(1 - second, p)
        pass_on(to_second(p))
    start, wait = exchange(
        me, n, grad_in, pl.ds(0, edge), pl.ds(padded_rows - edge, edge), from_up, from_down, edge_sems
    )
    start()
    for p in ranks + [rank]:
        add_pair(second, p)
    for p in ranks + [rank]:
        to_second(p).wait_recv()
        t3[p] = t2[second, p] + r2[p]
        if p is not rank:
            pass_on(remote(t3.at[p], r3.at[rank], out3.at[p], in3.at[rank], p * 4 + me % 4))

    loads[0].wait()
    power = jnp.zeros((length, length), jnp.float32)
    for k in range(2 * modes):
        p = probe[k * length : (k + 1) * length, :]
        power = power + p * p
    step = object_rate / jnp.max(power, axis=(0, 1), keepdims=True)
    loads[1].wait()
    loads[2].wait()
    base = margin if final else 0

    def out(s):
        return slice(s.start - base, s.stop - base)

    inner = slice(base + edge, padded_rows - base - edge)
    top = slice(base, base + edge)
    low = slice(padded_rows - base - edge, padded_rows - base)
    made[:, out(inner)] = obj[:, inner] - step * grad[:, inner]

    share = t3[rank]
    for p in ranks:
        remote(t3.at[p], r3.at[p], out3.at[p], in3.at[p], p * 4 + me % 4).wait_recv()
        share = share + r3[p]
    energy = jnp.sum(share[rows:], axis=(0, 1), keepdims=True)

    def region(c, b, p):
        return pl.ds(pl.multiple_of(c * half + b * quarter + p * rows, rows), rows)

    own = region(core, second, rank)
    fresh[own, :] = probe[own, :] - probe_rate * length * length / energy * share[:rows]

    def to_rank(p, q):
        part = fresh.at[region(core, second, q)]
        return remote(part, part, gout3.at[p], gin3.at[q], p * 4 + me % 4)

    def to_other(b, p):
        part = fresh.at[region(core, b, p)]
        return remote(part, part, gout2.at[p], gin2.at[p], other)

    def to_mate(c, b, p):
        part = fresh.at[region(c, b, p)]
        return remote(part, part, gout1.at[b * peers + p], gin1.at[b * peers + p], mate)

    for p in ranks:
        pass_on(to_rank(p, rank))
    pass_on(to_other(second, rank))
    pass_on(to_mate(core, second, rank))
    for p in ranks:
        to_rank(p, p).wait_recv()
        pass_on(to_other(second, p))
        pass_on(to_mate(core, second, p))

    wait()
    made[:, out(top)] = obj[:, top] - step * (grad[:, top] + from_up[...])
    made[:, out(low)] = obj[:, low] - step * (grad[:, low] + from_down[...])
    if not final:
        @pl.when(me == 0)
        def _():
            made[:, :margin] = jnp.zeros((2, margin, obj.shape[2]), jnp.float32)

        @pl.when(me == n - 1)
        def _():
            made[:, padded_rows - margin :] = jnp.zeros((2, margin, obj.shape[2]), jnp.float32)

    store = pltpu.make_async_copy(made, new_obj, local_sems.at[1])
    store.start()
    for p in [rank] + ranks:
        to_other(1 - second, p).wait_recv()
        pass_on(to_mate(core, 1 - second, p))
    for p in [rank] + ranks:
        to_mate(1 - core, second, p).wait_recv()
    for p in [rank] + ranks:
        to_mate(1 - core, 1 - second, p).wait_recv()
    result = pltpu.make_async_copy(fresh, new_probe, local_sems.at[0])
    result.start()
    for copy in sends:
        copy.wait_send()
    store.wait()
    result.wait()


def body(object_tile, probe_modes, measured, offsets, counts):
    n = lax.axis_size("row")
    parts, tile_rows, cols = object_tile.shape
    modes, length = probe_modes.shape[1], probe_modes.shape[2]
    margin = length // 2
    padded_rows = tile_rows + 2 * margin
    flat = 2 * modes * length
    half, quarter = flat // 2, flat // 4
    peers = n // 4
    rows = quarter // peers
    f32 = jnp.float32
    dma = pltpu.SemaphoreType.DMA
    padded_shape = jax.ShapeDtypeStruct((parts, padded_rows, cols), f32)
    tables = dft_tables(length)

    padded = pl.pallas_call(
        functools.partial(halo_kernel, n),
        name="halo",
        out_shape=padded_shape,
        in_specs=[VMEM],
        out_specs=VMEM,
        scratch_shapes=[pltpu.VMEM((parts, margin, cols), f32)] * 2 + [dma((4,))],
        compiler_params=pltpu.CompilerParams(collective_id=0, has_side_effects=True),
    )(object_tile)

    gradient = pl.pallas_call(
        gradient_kernel,
        name="gradient",
        out_shape=[padded_shape, jax.ShapeDtypeStruct((2, half + ENERGY_ROWS, length), f32)],
        in_specs=[SMEM, SMEM, VMEM, VMEM] + [ANY] * 5,
        out_specs=[VMEM, VMEM],
        scratch_shapes=[
            pltpu.VMEM((6 * length, modes * length), jnp.bfloat16),
            pltpu.VMEM((modes * length, 6 * length), jnp.bfloat16),
            pltpu.VMEM((modes * length, 2 * length), f32),
        ]
        + [pltpu.VMEM((parts, cols // length, padded_rows, length), f32)] * 2
        + [pltpu.VMEM(measured.shape, f32)]
        + [pltpu.VMEM(tables[i].shape, jnp.bfloat16) for i in (0, 3, 2, 1)]
        + [dma((5,))],
    )

    probe_now = probe_modes
    for sweep in range(ITERS):
        final = sweep == ITERS - 1
        edge = margin if final else 2 * margin
        grad, probe_grad = gradient(
            offsets.T, counts, padded, probe_now, measured, tables[0], tables[3], tables[2], tables[1]
        )
        padded, fresh = pl.pallas_call(
            functools.partial(update_kernel, n, final, modes),
            name="update_last" if final else "update",
            out_shape=[
                jax.ShapeDtypeStruct((parts, tile_rows if final else padded_rows, cols), f32),
                jax.ShapeDtypeStruct((flat, length), f32),
            ],
            in_specs=[ANY] * 3 + [VMEM],
            out_specs=[ANY] * 2,
            scratch_shapes=[
                pltpu.VMEM((parts, edge, cols), f32),
                pltpu.VMEM((parts, edge, cols), f32),
                pltpu.VMEM((parts, padded_rows, cols), f32),
                pltpu.VMEM((parts, padded_rows, cols), f32),
                pltpu.VMEM((parts, tile_rows if final else padded_rows, cols), f32),
                pltpu.VMEM((flat, length), f32),
                pltpu.VMEM((half + ENERGY_ROWS, length), f32),
                pltpu.VMEM((2, peers, rows + ENERGY_ROWS, length), f32),
                pltpu.VMEM((peers, rows + ENERGY_ROWS, length), f32),
                pltpu.VMEM((peers, rows + ENERGY_ROWS, length), f32),
                pltpu.VMEM((peers, rows + ENERGY_ROWS, length), f32),
                pltpu.VMEM((flat, length), f32),
                dma((3,)),
                dma((4,)),
                dma((2,)),
                dma((peers,)), dma((peers,)),
                dma((peers,)), dma((peers,)), dma((peers,)), dma((peers,)),
                dma((peers,)), dma((peers,)), dma((2 * peers,)), dma((2 * peers,)),
            ],
            compiler_params=pltpu.CompilerParams(
                collective_id=1 + sweep, has_side_effects=True
            ),
        )(padded, grad, probe_now.reshape(flat, length), probe_grad)
        probe_now = fresh.reshape(probe_modes.shape)
    return (padded, probe_now)


def solution(mesh):
    return jax.shard_map(
        body,
        mesh=mesh,
        in_specs=(
            P(None, ("parts", "row"), None),
            P(),
            P(("parts", "row"), None, None),
            P(("parts", "row"), None),
            P(("parts", "row")),
        ),
        out_specs=(P(None, ("parts", "row"), None), P("parts", None, None, None)),
        check_vma=False,
    )
```

```python
import functools
import math

import jax
import jax.numpy as jnp
import numpy as np
from jax import lax
from jax.experimental import pallas as pl
from jax.experimental.pallas import tpu as pltpu
from jax.sharding import PartitionSpec as P

ITERS = 2
object_rate = 0.2
probe_rate = 0.5
ENERGY_ROWS = 8
VMEM = pl.BlockSpec(memory_space=pltpu.VMEM)
ANY = pl.BlockSpec(memory_space=pl.ANY)
SMEM = pl.BlockSpec(memory_space=pltpu.SMEM)
MESH = pl.DeviceIdType.MESH


def dft_tables(length):
    index = np.arange(length)
    phase = 2.0 * math.pi / length * (index[:, None] * index[None, :] % length)
    cosine = np.cos(phase) / math.sqrt(length)
    sine = -np.sin(phase) / math.sqrt(length)
    forward = np.block([[cosine, -sine], [sine, cosine]]).astype(np.float32)
    backward = np.block([[cosine, sine], [-sine, cosine]]).astype(np.float32)
    tables = []
    for table in (forward, backward):
        high = table.astype(jnp.bfloat16)
        low = (table - high.astype(np.float32)).astype(jnp.bfloat16)
        tables.append(jnp.asarray(np.concatenate([high, high, low], axis=1)))
        tables.append(jnp.asarray(np.concatenate([high, high, low], axis=0)))
    return tables


def halves(x):
    high = x.astype(jnp.bfloat16)
    return high, (x - high.astype(jnp.float32)).astype(jnp.bfloat16)


def gradient_kernel(
    offsets, counts, obj, probe, measured, left_f, right_f, left_b, right_b,
    grad, probe_grad, x3, y3, far, columns, sums,
):
    slots, length = measured.shape[0], measured.shape[1]
    modes = probe.shape[1]
    cols = obj.shape[2]
    margin = length // 2
    half = modes * length
    blocks = range(cols // length)
    for c in range(obj.shape[0]):
        for j in blocks:
            columns[c, j] = obj[c, :, j * length : (j + 1) * length]
    sums[...] = jnp.zeros_like(sums)
    probe_grad[...] = jnp.zeros_like(probe_grad)
    wide = 2 * length

    def put_x(k, part, value):
        high, low = halves(value)
        c = pl.ds(k * length, length)
        x3[pl.ds(part * length, length), c] = high
        x3[pl.ds(wide + part * length, length), c] = low
        x3[pl.ds(2 * wide + part * length, length), c] = high

    def put_y(k, part, value):
        high, low = halves(value)
        r = pl.ds(k * length, length)
        y3[r, pl.ds(part * length, length)] = high
        y3[r, pl.ds(wide + part * length, length)] = low
        y3[r, pl.ds(2 * wide + part * length, length)] = high

    def visit(s, carry):
        row = offsets[0, s] + margin
        col = offsets[1, s]
        shift = lax.rem(cols - col, cols)

        def cut(c):
            whole = jnp.concatenate([columns[c, j, pl.ds(row, length), :] for j in blocks], axis=1)
            return pltpu.roll(whole, shift, 1)[:, :length]

        wr, wi = cut(0), cut(1)
        energy = (wr * wr + wi * wi).reshape(-1, ENERGY_ROWS, length).sum(axis=0)
        probe_grad[0, half:, :] += energy
        probe_grad[1, half:, :] += energy
        for k in range(modes):
            pr, pi = probe[0, k], probe[1, k]
            put_x(k, 0, pr * wr - pi * wi)
            put_x(k, 1, pr * wi + pi * wr)
        left = jnp.dot(left_f[...], x3[...], preferred_element_type=jnp.float32)
        for k in range(modes):
            for part in range(2):
                put_y(k, part, left[part * length : (part + 1) * length, k * length : (k + 1) * length])
        far[...] = jnp.dot(y3[...], right_f[...], preferred_element_type=jnp.float32)
        intensity = jnp.zeros((length, length), jnp.float32)
        for k in range(modes):
            fr = far[k * length : (k + 1) * length, :length]
            fi = far[k * length : (k + 1) * length, length:]
            intensity = intensity + (fr * fr + fi * fi)
        resid = intensity - measured[s]
        for k in range(modes):
            for part in range(2):
                put_y(
                    k, part,
                    resid * far[k * length : (k + 1) * length, part * length : (part + 1) * length],
                )
        right = jnp.dot(y3[...], right_b[...], preferred_element_type=jnp.float32)
        for k in range(modes):
            for part in range(2):
                put_x(k, part, right[k * length : (k + 1) * length, part * length : (part + 1) * length])
        back = jnp.dot(left_b[...], x3[...], preferred_element_type=jnp.float32)
        gr = jnp.zeros((length, length), jnp.float32)
        gi = jnp.zeros((length, length), jnp.float32)
        wr, wi = cut(0), cut(1)
        for k in range(modes):
            pr, pi = probe[0, k], probe[1, k]
            br = back[:length, k * length : (k + 1) * length]
            bi = back[length:, k * length : (k + 1) * length]
            gr = gr + (pr * br + pi * bi)
            gi = gi + (pr * bi - pi * br)
            probe_grad[0, k * length : (k + 1) * length, :] += wr * br + wi * bi
            probe_grad[1, k * length : (k + 1) * length, :] += wr * bi - wi * br
        rest = jnp.zeros((length, cols - length), jnp.float32)
        for c, g in ((0, gr), (1, gi)):
            placed = pltpu.roll(jnp.concatenate([g, rest], axis=1), col, 1)
            for j in blocks:
                sums[c, j, pl.ds(row, length), :] += placed[:, j * length : (j + 1) * length]
        return carry

    lax.fori_loop(0, jnp.minimum(counts[0], slots), visit, 0)
    for c in range(obj.shape[0]):
        for j in blocks:
            grad[c, :, j * length : (j + 1) * length] = sums[c, j]


def greet(me, n, devices):
    barrier = pltpu.get_barrier_semaphore()

    def signal(device):
        pl.semaphore_signal(barrier, inc=1, device_id={"row": device}, device_id_type=MESH)

    pl.when(me > 0)(lambda: signal(me - 1))
    pl.when(me < n - 1)(lambda: signal(me + 1))
    for device in devices:
        signal(device)
    inside = (me > 0) & (me < n - 1)
    pl.when(inside)(lambda: pl.semaphore_wait(barrier, len(devices) + 2))
    pl.when(jnp.logical_not(inside))(lambda: pl.semaphore_wait(barrier, len(devices) + 1))


def remote(src, dst, send, recv, device):
    return pltpu.make_async_remote_copy(
        src_ref=src, dst_ref=dst, send_sem=send, recv_sem=recv,
        device_id={"row": device}, device_id_type=MESH,
    )


def exchange(me, n, array, rows_up, rows_down, from_up, from_down, sems):
    up = remote(array.at[:, rows_up], from_down, sems.at[0], sems.at[1], me - 1)
    down = remote(array.at[:, rows_down], from_up, sems.at[2], sems.at[3], me + 1)

    def start():
        pl.when(me > 0)(up.start)
        pl.when(me < n - 1)(down.start)

    def wait():
        @pl.when(me > 0)
        def _():
            up.wait_send()
            down.wait_recv()

        @pl.when(me < n - 1)
        def _():
            down.wait_send()
            up.wait_recv()

    return start, wait


def halo_kernel(n, tile, padded, from_up, from_down, sems):
    me = lax.axis_index("row")
    rows = tile.shape[1]
    margin = from_up.shape[1]
    greet(me, n, [])
    start, wait = exchange(
        me, n, tile, pl.ds(0, margin), pl.ds(rows - margin, margin), from_up, from_down, sems
    )
    start()
    padded[:, margin : margin + rows] = tile[...]

    @pl.when(me == 0)
    def _():
        padded[:, :margin] = jnp.zeros_like(from_up)

    @pl.when(me == n - 1)
    def _():
        padded[:, margin + rows :] = jnp.zeros_like(from_down)

    wait()

    @pl.when(me > 0)
    def _():
        padded[:, :margin] = from_up[...]

    @pl.when(me < n - 1)
    def _():
        padded[:, margin + rows :] = from_down[...]


def update_kernel(
    n, final, modes, obj_in, grad_in, probe_in, probe_grad, new_obj, new_probe,
    from_up, from_down, obj, grad, made, probe, r1, t2, r2, t3, r3, fresh,
    local_sems, edge_sems, pair_sems, out2, in2,
    out3, in3, gout3, gin3, gout2, gin2, gout1, gin1,
):
    me = lax.axis_index("row")
    length = probe.shape[1]
    margin = length // 2
    padded_rows = obj.shape[1]
    edge = from_up.shape[1]
    peers = t3.shape[0]
    rows = t3.shape[1] - ENERGY_ROWS
    half, quarter = probe.shape[0] // 2, probe.shape[0] // 4
    core = me % 2
    second = (me // 2) % 2
    rank = me // 4
    mate = me + 1 - 2 * core
    other = me + 2 - 4 * second
    ranks = [(rank + d) % peers for d in range(1, peers)]
    loads = [
        pltpu.make_async_copy(src, dst, local_sems.at[i])
        for i, (src, dst) in enumerate(((probe_in, probe), (obj_in, obj), (grad_in, grad)))
    ]
    for load in loads:
        load.start()
    greet(me, n, [mate, other] + [p * 4 + me % 4 for p in ranks])
    one = remote(probe_grad.at[1 - core], r1, pair_sems.at[0], pair_sems.at[1], mate)
    one.start()

    @pl.when(me == 0)
    def _():
        from_up[...] = jnp.zeros_like(from_up)

    @pl.when(me == n - 1)
    def _():
        from_down[...] = jnp.zeros_like(from_down)

    one.wait_recv()

    def add_pair(b, p):
        part = pl.ds(pl.multiple_of(b * quarter + p * rows, rows), rows)
        t2[b, p, :rows] = probe_grad[core, part] + r1[part]
        t2[b, p, rows:] = probe_grad[core, half:] + r1[half:]

    sends = [one]

    def pass_on(copy):
        copy.start()
        sends.append(copy)

    def to_second(p):
        return remote(t2.at[1 - second, p], r2.at[p], out2.at[p], in2.at[p], other)

    for p in ranks + [rank]:
        add_pair(1 - second, p)
        pass_on(to_second(p))
    start, wait = exchange(
        me, n, grad_in, pl.ds(0, edge), pl.ds(padded_rows - edge, edge), from_up, from_down, edge_sems
    )
    start()
    for p in ranks + [rank]:
        add_pair(second, p)
    for p in ranks + [rank]:
        to_second(p).wait_recv()
        t3[p] = t2[second, p] + r2[p]
        if p is not rank:
            pass_on(remote(t3.at[p], r3.at[rank], out3.at[p], in3.at[rank], p * 4 + me % 4))

    loads[0].wait()
    power = jnp.zeros((length, length), jnp.float32)
    for k in range(2 * modes):
        p = probe[k * length : (k + 1) * length, :]
        power = power + p * p
    step = object_rate / jnp.max(power, axis=(0, 1), keepdims=True)
    loads[1].wait()
    loads[2].wait()
    base = margin if final else 0

    def out(s):
        return slice(s.start - base, s.stop - base)

    inner = slice(base + edge, padded_rows - base - edge)
    top = slice(base, base + edge)
    low = slice(padded_rows - base - edge, padded_rows - base)
    made[:, out(inner)] = obj[:, inner] - step * grad[:, inner]

    share = t3[rank]
    for p in ranks:
        remote(t3.at[p], r3.at[p], out3.at[p], in3.at[p], p * 4 + me % 4).wait_recv()
        share = share + r3[p]
    energy = jnp.sum(share[rows:], axis=(0, 1), keepdims=True)

    def region(c, b, p):
        return pl.ds(pl.multiple_of(c * half + b * quarter + p * rows, rows), rows)

    own = region(core, second, rank)
    fresh[own, :] = probe[own, :] - probe_rate * length * length / energy * share[:rows]

    def to_rank(p, q):
        part = fresh.at[region(core, second, q)]
        return remote(part, part, gout3.at[p], gin3.at[q], p * 4 + me % 4)

    def to_other(b, p):
        part = fresh.at[region(core, b, p)]
        return remote(part, part, gout2.at[p], gin2.at[p], other)

    def to_mate(c, b, p):
        part = fresh.at[region(c, b, p)]
        return remote(part, part, gout1.at[b * peers + p], gin1.at[b * peers + p], mate)

    for p in ranks:
        pass_on(to_rank(p, rank))
    pass_on(to_other(second, rank))
    pass_on(to_mate(core, second, rank))
    for p in ranks:
        to_rank(p, p).wait_recv()
        pass_on(to_other(second, p))
        pass_on(to_mate(core, second, p))

    wait()
    made[:, out(top)] = obj[:, top] - step * (grad[:, top] + from_up[...])
    made[:, out(low)] = obj[:, low] - step * (grad[:, low] + from_down[...])
    if not final:
        @pl.when(me == 0)
        def _():
            made[:, :margin] = jnp.zeros((2, margin, obj.shape[2]), jnp.float32)

        @pl.when(me == n - 1)
        def _():
            made[:, padded_rows - margin :] = jnp.zeros((2, margin, obj.shape[2]), jnp.float32)

    store = pltpu.make_async_copy(made, new_obj, local_sems.at[1])
    store.start()
    for p in [rank] + ranks:
        to_other(1 - second, p).wait_recv()
        pass_on(to_mate(core, 1 - second, p))
    for p in [rank] + ranks:
        to_mate(1 - core, second, p).wait_recv()
    for p in [rank] + ranks:
        to_mate(1 - core, 1 - second, p).wait_recv()
    result = pltpu.make_async_copy(fresh, new_probe, local_sems.at[0])
    result.start()
    for copy in sends:
        copy.wait_send()
    store.wait()
    result.wait()


def body(object_tile, probe_modes, measured, offsets, counts):
    n = lax.axis_size("row")
    parts, tile_rows, cols = object_tile.shape
    modes, length = probe_modes.shape[1], probe_modes.shape[2]
    margin = length // 2
    padded_rows = tile_rows + 2 * margin
    flat = 2 * modes * length
    half, quarter = flat // 2, flat // 4
    peers = n // 4
    rows = quarter // peers
    f32 = jnp.float32
    dma = pltpu.SemaphoreType.DMA
    padded_shape = jax.ShapeDtypeStruct((parts, padded_rows, cols), f32)
    tables = dft_tables(length)

    padded = pl.pallas_call(
        functools.partial(halo_kernel, n),
        name="halo",
        out_shape=padded_shape,
        in_specs=[VMEM],
        out_specs=VMEM,
        scratch_shapes=[pltpu.VMEM((parts, margin, cols), f32)] * 2 + [dma((4,))],
        compiler_params=pltpu.CompilerParams(collective_id=0, has_side_effects=True),
    )(object_tile)

    gradient = pl.pallas_call(
        gradient_kernel,
        name="gradient",
        out_shape=[padded_shape, jax.ShapeDtypeStruct((2, half + ENERGY_ROWS, length), f32)],
        in_specs=[SMEM, SMEM] + [VMEM] * 7,
        out_specs=[VMEM, VMEM],
        scratch_shapes=[
            pltpu.VMEM((6 * length, modes * length), jnp.bfloat16),
            pltpu.VMEM((modes * length, 6 * length), jnp.bfloat16),
            pltpu.VMEM((modes * length, 2 * length), f32),
        ]
        + [pltpu.VMEM((parts, cols // length, padded_rows, length), f32)] * 2,
    )

    probe_now = probe_modes
    for sweep in range(ITERS):
        final = sweep == ITERS - 1
        edge = margin if final else 2 * margin
        grad, probe_grad = gradient(
            offsets.T, counts, padded, probe_now, measured, tables[0], tables[3], tables[2], tables[1]
        )
        padded, fresh = pl.pallas_call(
            functools.partial(update_kernel, n, final, modes),
            name="update_last" if final else "update",
            out_shape=[
                jax.ShapeDtypeStruct((parts, tile_rows if final else padded_rows, cols), f32),
                jax.ShapeDtypeStruct((flat, length), f32),
            ],
            in_specs=[ANY] * 3 + [VMEM],
            out_specs=[ANY] * 2,
            scratch_shapes=[
                pltpu.VMEM((parts, edge, cols), f32),
                pltpu.VMEM((parts, edge, cols), f32),
                pltpu.VMEM((parts, padded_rows, cols), f32),
                pltpu.VMEM((parts, padded_rows, cols), f32),
                pltpu.VMEM((parts, tile_rows if final else padded_rows, cols), f32),
                pltpu.VMEM((flat, length), f32),
                pltpu.VMEM((half + ENERGY_ROWS, length), f32),
                pltpu.VMEM((2, peers, rows + ENERGY_ROWS, length), f32),
                pltpu.VMEM((peers, rows + ENERGY_ROWS, length), f32),
                pltpu.VMEM((peers, rows + ENERGY_ROWS, length), f32),
                pltpu.VMEM((peers, rows + ENERGY_ROWS, length), f32),
                pltpu.VMEM((flat, length), f32),
                dma((3,)),
                dma((4,)),
                dma((2,)),
                dma((peers,)), dma((peers,)),
                dma((peers,)), dma((peers,)), dma((peers,)), dma((peers,)),
                dma((peers,)), dma((peers,)), dma((2 * peers,)), dma((2 * peers,)),
            ],
            compiler_params=pltpu.CompilerParams(
                collective_id=1 + sweep, has_side_effects=True
            ),
        )(padded, grad, probe_now.reshape(flat, length), probe_grad)
        probe_now = fresh.reshape(probe_modes.shape)
    return (padded, probe_now)


def solution(mesh):
    return jax.shard_map(
        body,
        mesh=mesh,
        in_specs=(
            P(None, ("parts", "row"), None),
            P(),
            P(("parts", "row"), None, None),
            P(("parts", "row"), None),
            P(("parts", "row")),
        ),
        out_specs=(P(None, ("parts", "row"), None), P("parts", None, None, None)),
        check_vma=False,
    )
```
